256 devices in a mesh: grp: 8 (over z_hi, x), sub: 32 (over z_lo, y, core).
Axes of the slice: x: 4, y: 4, z: 8 (z_hi: 2, z_lo: 4; z = z_hi * 4 + z_lo), core: 2. Of those that a mesh axis runs over, the one named last changes fastest.
Arguments:
- counts: int32 [256], P(('grp', 'sub')), may hold values from 1 to 3, as said below
- block_map: int32 [768], P(('grp', 'sub')), may hold values from 0 to 31
- perms: int32 [768, 256], P(('grp', 'sub')), may hold values from 0 to 255, each once within a row
- mass_ii: bfloat16 [768, 1024, 1024], P(('grp', 'sub')), may hold values from -0.005859375 to 0.005859375
- mass_ib: bfloat16 [768, 1024, 256], P(('grp', 'sub')), may hold values from -0.1875 to 0.1875
- mass_bb: bfloat16 [768, 256, 256], P(('grp', 'sub')), may hold values from -6 to 6
- constraint_modes: bfloat16 [768, 1024, 256], P(('grp', 'sub')), may hold values from -6 to 6
- fixed_modes: bfloat16 [768, 1024, 128], P(('grp', 'sub')), may hold values from -6 to 6
Outputs:
- blocks: float32 [128, 256, 256], P('grp', 'sub')
- coupling: float32 [768, 128, 256], P(('grp', 'sub'))
The draws below stay inside these ranges and needn't reach their ends.
Inputs may be any that keep to these rules, and one draw needn't show every extreme that they name: `counts`: at least one device uses all 3 slots and one uses a single slot.
All inputs are finite; a program needn't handle non-finite values.
Results may differ from the reference program's by a relative error of at most 0.0021.
Values sent between devices are 32-bit elements; how exact they have to be, the bound alone decides.
A program may use at most 128 MiB of HBM per device.

```python
import jax
import jax.numpy as jnp
from jax import lax

I = 1024
B = 256
K = 128
SLOTS = 3
NBG = 16
CAP = 768
N_GRP = 8
N_SUB = 32
DEVICES = 256


def draw_counts(key, part):
    raw = jax.random.randint(key, (DEVICES,), 0, 6)
    values = jnp.where(raw < 4, 1, jnp.where(raw == 4, 2, SLOTS))
    values = jnp.minimum(values, SLOTS)
    values = values.at[0].set(SLOTS).at[1].set(1)
    return values.astype(jnp.int32)


def place_ends(drawn, own_key, low, high):
    extent = drawn.shape
    place = [jax.random.randint(jax.random.fold_in(own_key, axis), (), 0, extent[axis]) for axis in range(len(extent))]
    drawn = drawn.at[tuple(place)].set(low)
    longest = extent.index(max(extent))
    place[longest] = (place[longest] + 1) % extent[longest]
    return drawn.at[tuple(place)].set(high)


def shard_levels(stream_key, shape, cuts, low, high):
    level, own = 1.0, jax.random.fold_in(stream_key, 6)
    for axis_at, parts in cuts:
        heights = jnp.exp(jax.random.uniform(jax.random.fold_in(own, axis_at), (parts,), jnp.float32, low / len(cuts), high / len(cuts)))
        level = level * jnp.repeat(heights, shape[axis_at] // parts).reshape([-1 if axis == axis_at else 1 for axis in range(len(shape))])
    return level


def scatter_about(key, extent, deviation, bound, shards=(), held_as=jnp.bfloat16):
    drawn = jax.random.normal(key, extent, jnp.float32) * deviation
    if len(shards) > 0:
        drawn = shard_levels(key, extent, shards, -0.22, 0.18) * drawn
    return jnp.clip(drawn, min=-bound, max=bound).astype(held_as)


def setup_inputs(seed: int = 0) -> dict:
    keys = jax.random.split(jax.random.key(seed), 9)
    return {
        "counts": draw_counts(jax.random.fold_in(keys[8], 71), 0),
        "block_map": place_ends(jax.random.randint(keys[1], (CAP,), 0, 2 * NBG), jax.random.fold_in(keys[1], 1), 0, (2 * NBG) - 1).astype(jnp.int32),
        "perms": jax.vmap(lambda own: jax.random.permutation(own, B))(jax.random.split(keys[2], CAP)).reshape((CAP, B)).astype(jnp.int32),
        "mass_ii": scatter_about(keys[3], (CAP, I, I), (I * I) ** -0.5, 0.005859375, ((0, 256),)),
        "mass_ib": scatter_about(keys[4], (CAP, I, B), I ** -0.5, 0.1875, ((0, 256),)),
        "mass_bb": scatter_about(keys[5], (CAP, B, B), 1.0, 6.0, ((0, 256),)),
        "constraint_modes": scatter_about(keys[6], (CAP, I, B), 1.0, 6.0, ((0, 256),)),
        "fixed_modes": scatter_about(keys[7], (CAP, I, K), 1.0, 6.0, ((0, 256),)),
    }


def contract(left, right):
    return lax.dot_general(left, right, (((0,), (0,)), ((), ())), preferred_element_type=jnp.float32)


def reduce_slot(mass_ii, mass_ib, mass_bb, constraint_modes, fixed_modes):
    product = jnp.dot(mass_ii, constraint_modes, preferred_element_type=jnp.float32).astype(jnp.bfloat16)
    cross = contract(constraint_modes, mass_ib)
    reduced = contract(constraint_modes, product) + cross + cross.T + mass_bb.astype(jnp.float32)
    coupled = contract(fixed_modes, product) + contract(fixed_modes, mass_ib)
    return reduced, coupled


def reference(counts, block_map, perms, mass_ii, mass_ib, mass_bb, constraint_modes, fixed_modes):
    width = mass_bb.shape[1]
    total_slots = mass_ii.shape[0]
    modes = fixed_modes.shape[2]

    def step(carry_blocks, items):
        slot_id, code, perm_row, m_ii, m_ib, m_bb, psi_slot, phi_slot = items
        device = slot_id // SLOTS
        used_flag = (slot_id % SLOTS) < counts[device]
        group_index = device // N_SUB

        def active_branch(unused):
            return reduce_slot(m_ii, m_ib, m_bb, psi_slot, phi_slot)

        def empty_branch(unused):
            return (jnp.zeros((width, width), jnp.float32), jnp.zeros((modes, width), jnp.float32))

        reduced, coupled = lax.cond(used_flag, active_branch, empty_branch, 0)
        target = ((group_index + code // NBG) % N_GRP) * NBG + code % NBG
        inverse = jnp.zeros((width,), jnp.int32).at[perm_row].set(jnp.arange(width, dtype=jnp.int32))
        placed = reduced[inverse][:, inverse]
        carry_blocks = carry_blocks.at[target.astype(jnp.int32)].add(placed)
        return carry_blocks, coupled

    start = jnp.zeros((NBG * N_GRP, width, width), jnp.float32)
    items = (jnp.arange(total_slots, dtype=jnp.int32), block_map, perms, mass_ii, mass_ib, mass_bb, constraint_modes, fixed_modes)
    blocks, coupling = lax.scan(step, start, items)
    return blocks, coupling
```

```python
import functools

import jax
import jax.numpy as jnp
from jax import lax
from jax.experimental import pallas as pl
from jax.experimental.pallas import tpu as pltpu
from jax.sharding import PartitionSpec as P

NBG = 16
X_CHIPS = 4
Z_RUN = 4
MESH = pl.DeviceIdType.MESH
HALVES = 2
LANES = 128


def contract(left, right):
    return lax.dot_general(left, right, (((0,), (0,)), ((), ())), preferred_element_type=jnp.float32)


def split(value):
    high = value.astype(jnp.bfloat16)
    low = (value - high.astype(jnp.float32)).astype(jnp.bfloat16)
    return high, low


def body(
    n_grp,
    n_sub,
    counts,
    codes_in,
    perms,
    mass_ii,
    mass_ib,
    mass_bb,
    modes,
    fixed,
    blocks,
    coupling,
    m_buf,
    pi_buf,
    b_buf,
    c_buf,
    f_buf,
    perm_buf,
    placed,
    rows_in,
    code_row,
    code_in,
    acc,
    staged,
    ahead_in,
    home_in,
    coup_buf,
    block_buf,
    load_sem,
    half_sem,
    out_sem,
    row_send,
    row_recv,
    code_sem,
    end_sem,
):
    slots, inner, width = mass_ib.shape
    own = width // n_sub
    grp = lax.axis_index("grp")
    sub = lax.axis_index("sub")
    run = n_sub // Z_RUN

    def mirrored(device):
        return (Z_RUN - 1 - device // run) * run + lax.rem(device, run)

    last = lax.rem(grp, X_CHIPS) == X_CHIPS - 1
    first = lax.rem(grp, X_CHIPS) == 0
    next_grp = lax.rem(grp + 1, n_grp)
    prev_grp = lax.rem(grp + n_grp - 1, n_grp)
    out_sub = jnp.where(last, mirrored(sub), sub)
    in_sub = jnp.where(first, mirrored(sub), sub)

    def loads(j):
        half = inner // HALVES
        copies = [pltpu.make_async_copy(modes.at[j], c_buf.at[j], load_sem.at[j, 0])]
        for part in range(HALVES):
            rows = pl.ds(part * half, half)
            copies.append(pltpu.make_async_copy(mass_ii.at[j, rows], m_buf.at[j, rows], half_sem.at[j, part]))
        copies.append(pltpu.make_async_copy(mass_ib.at[j], pi_buf.at[j, :, pl.ds(width, width)], load_sem.at[j, 1]))
        copies.append(pltpu.make_async_copy(mass_bb.at[j], b_buf.at[j], load_sem.at[j, 2]))
        copies.append(pltpu.make_async_copy(fixed.at[j], f_buf.at[j], load_sem.at[j, 3]))
        return copies

    for copy in loads(0):
        copy.start()
    perm_copy = pltpu.make_async_copy(perms, perm_buf, load_sem.at[0, 4])
    perm_copy.start()

    barrier = pltpu.get_barrier_semaphore()

    def greet(step, carry):
        peer = lax.rem(sub + step, n_sub)
        pl.semaphore_signal(barrier, inc=1, device_id={"sub": peer}, device_id_type=MESH)
        return carry

    lax.fori_loop(1, n_sub, greet, 0)
    pl.semaphore_signal(barrier, inc=1, device_id={"grp": next_grp, "sub": out_sub}, device_id_type=MESH)
    pl.semaphore_signal(barrier, inc=1, device_id={"grp": prev_grp, "sub": in_sub}, device_id_type=MESH)

    used = counts[0]
    lane = lax.broadcasted_iota(jnp.int32, (1, 128), 1)
    row = jnp.full((1, 128), -1, jnp.int32)
    for j in range(slots):
        row = jnp.where((lane == j) & (j < used), codes_in[j], row)
    code_row[...] = row
    code_in[0] = row

    def code_copy(step):
        peer = lax.rem(sub + step, n_sub)
        return pltpu.make_async_remote_copy(
            src_ref=code_row,
            dst_ref=code_in.at[step],
            send_sem=code_sem.at[0],
            recv_sem=code_sem.at[1],
            device_id={"sub": peer},
            device_id_type=MESH,
        )

    def rows_copy(j, step):
        peer = lax.rem(sub + step, n_sub)
        block = jnp.where(last, mirrored(peer), peer)
        return pltpu.make_async_remote_copy(
            src_ref=placed.at[j, :, pl.ds(pl.multiple_of(block * own, own), own)],
            dst_ref=rows_in.at[j, :, pl.ds(pl.multiple_of(step * own, own), own)],
            send_sem=row_send.at[j],
            recv_sem=row_recv.at[j],
            device_id={"sub": peer},
            device_id_type=MESH,
        )

    perm_copy.wait()
    row_of = lax.broadcasted_iota(jnp.int32, (width, width), 0)

    def slot(j, carry):
        ready = loads(j)
        half = inner // HALVES
        ready[0].wait()
        for part in range(HALVES):
            ready[1 + part].wait()
            if part == HALVES - 1:

                @pl.when(j + 1 < slots)
                def _():
                    for copy in loads(j + 1):
                        copy.start()

            rows = pl.ds(part * half, half)
            pi_buf[j, rows, pl.ds(0, width)] = jnp.dot(
                m_buf[j, rows], c_buf[j], preferred_element_type=jnp.float32
            ).astype(jnp.bfloat16)
        ready[1 + HALVES].wait()
        ready[2 + HALVES].wait()
        both = contract(c_buf[j], pi_buf[j])
        cross = both[:, width:]
        reduced = both[:, :width] + cross + cross.T + b_buf[j].astype(jnp.float32)
        hot = (row_of == perm_buf[pl.ds(j, 1), :]).astype(jnp.float32).astype(jnp.bfloat16)
        high, low = split(reduced)
        moved_high = jnp.dot(hot, high, preferred_element_type=jnp.float32).astype(jnp.bfloat16)
        moved_low = jnp.dot(hot, low, preferred_element_type=jnp.float32).astype(jnp.bfloat16)
        across = (((1,), (1,)), ((), ()))
        moved = lax.dot_general(
            moved_high, hot, across, preferred_element_type=jnp.float32
        ) + lax.dot_general(moved_low, hot, across, preferred_element_type=jnp.float32)
        for side in range(width // LANES):
            placed[j, side] = moved[:, side * LANES : (side + 1) * LANES]

        @pl.when(j == 0)
        def _():
            pl.semaphore_wait(barrier, n_sub + 1)
            lax.fori_loop(1, n_sub, lambda step, c: (code_copy(step).start(), c)[1], 0)

        lax.fori_loop(1, n_sub, lambda step, c: (rows_copy(j, step).start(), c)[1], 0)
        mine = pl.ds(pl.multiple_of(out_sub * own, own), own)
        rows_in[j, :, pl.ds(0, own)] = placed[j, :, mine]

        ready[3 + HALVES].wait()
        pair = contract(f_buf[j], pi_buf[j])
        coupled = pair[:, :width] + pair[:, width:]
        coup_buf[j] = jnp.where(j < used, coupled, 0.0)
        pltpu.make_async_copy(coup_buf.at[j], coupling.at[j], out_sem.at[j]).start()
        return carry

    lax.fori_loop(0, slots, slot, 0)

    others = pltpu.make_async_remote_copy(
        src_ref=code_in.at[pl.ds(1, n_sub - 1)],
        dst_ref=code_in.at[pl.ds(1, n_sub - 1)],
        send_sem=code_sem.at[0],
        recv_sem=code_sem.at[1],
        device_id={"sub": sub},
        device_id_type=MESH,
    )
    others.wait_send()
    others.wait_recv()
    code_all = code_in[...].reshape(n_sub, 128)
    target = lax.broadcasted_iota(jnp.int32, (n_sub, 2 * NBG), 1)
    for j in range(slots):
        rest = pl.ds(own, width - own)
        arrived = pltpu.make_async_remote_copy(
            src_ref=rows_in.at[j, :, rest],
            dst_ref=rows_in.at[j, :, rest],
            send_sem=row_send.at[j],
            recv_sem=row_recv.at[j],
            device_id={"sub": sub},
            device_id_type=MESH,
        )
        arrived.wait_recv()
        arrived.wait_send()
        hot = (code_all[:, j : j + 1] == target).astype(jnp.float32).astype(jnp.bfloat16)
        hot = jnp.concatenate([hot, hot], axis=0)
        for r in range(own):
            for side in range(width // LANES):
                high, low = split(rows_in[j, side, pl.ds(r, n_sub, stride=own), :])
                part = contract(hot, jnp.concatenate([high, low], axis=0))
                if j > 0:
                    part = part + acc[r, side]
                if j < slots - 1:
                    acc[r, side] = part
                else:
                    staged[side, pl.ds(r, 2 * NBG, stride=own), :] = part

    size = NBG * own
    ahead = pltpu.make_async_remote_copy(
        src_ref=staged.at[:, pl.ds(size, size)],
        dst_ref=ahead_in,
        send_sem=end_sem.at[0],
        recv_sem=end_sem.at[1],
        device_id={"grp": next_grp, "sub": out_sub},
        device_id_type=MESH,
    )
    ahead.start()
    home = pltpu.make_async_remote_copy(
        src_ref=staged.at[:, pl.ds(0, size)],
        dst_ref=home_in,
        send_sem=end_sem.at[2],
        recv_sem=end_sem.at[3],
        device_id={"sub": out_sub},
        device_id_type=MESH,
    )

    @pl.when(last)
    def _():
        home.start()
        home.wait()

    @pl.when(jnp.logical_not(last))
    def _():
        home_in[...] = staged[:, pl.ds(0, size)]

    ahead.wait()
    for side in range(width // LANES):
        block_buf[:, :, pl.ds(side * LANES, LANES)] = (home_in[side] + ahead_in[side]).reshape(NBG, own, LANES)
    out = pltpu.make_async_copy(block_buf, blocks, out_sem.at[slots])
    out.start()
    for j in range(slots):
        pltpu.make_async_copy(coup_buf.at[j], coupling.at[j], out_sem.at[j]).wait()
    out.wait()


def solution(mesh):
    n_grp, n_sub = mesh.shape["grp"], mesh.shape["sub"]

    def per_device(counts, block_map, perms, mass_ii, mass_ib, mass_bb, modes, fixed):
        slots, inner, width = mass_ib.shape
        k = fixed.shape[2]
        own = width // n_sub
        anywhere = pl.BlockSpec(memory_space=pl.ANY)
        smem = pl.BlockSpec(memory_space=pltpu.SMEM)
        flops = 2 * slots * inner * width * (inner + 2 * width + 2 * k)
        return pl.pallas_call(
            functools.partial(body, n_grp, n_sub),
            out_shape=(
                jax.ShapeDtypeStruct((NBG, own, width), jnp.float32),
                jax.ShapeDtypeStruct((slots, k, width), jnp.float32),
            ),
            in_specs=[smem, smem] + [anywhere] * 6,
            out_specs=(anywhere, anywhere),
            scratch_shapes=[
                pltpu.VMEM((slots, inner, inner), jnp.bfloat16),
                pltpu.VMEM((slots, inner, 2 * width), jnp.bfloat16),
                pltpu.VMEM((slots, width, width), jnp.bfloat16),
                pltpu.VMEM((slots, inner, width), jnp.bfloat16),
                pltpu.VMEM((slots, inner, k), jnp.bfloat16),
                pltpu.VMEM((slots, width), jnp.int32),
                pltpu.VMEM((slots, width // LANES, width, LANES), jnp.float32),
                pltpu.VMEM((slots, width // LANES, width, LANES), jnp.float32),
                pltpu.VMEM((1, 128), jnp.int32),
                pltpu.VMEM((n_sub, 1, 128), jnp.int32),
                pltpu.VMEM((own, width // LANES, 2 * NBG, LANES), jnp.float32),
                pltpu.VMEM((width // LANES, 2 * NBG * own, LANES), jnp.float32),
                pltpu.VMEM((width // LANES, NBG * own, LANES), jnp.float32),
                pltpu.VMEM((width // LANES, NBG * own, LANES), jnp.float32),
                pltpu.VMEM((slots, k, width), jnp.float32),
                pltpu.VMEM((NBG, own, width), jnp.float32),
                pltpu.SemaphoreType.DMA((slots, 5)),
                pltpu.SemaphoreType.DMA((slots, HALVES)),
                pltpu.SemaphoreType.DMA((slots + 1,)),
                pltpu.SemaphoreType.DMA((slots,)),
                pltpu.SemaphoreType.DMA((slots,)),
                pltpu.SemaphoreType.DMA((2,)),
                pltpu.SemaphoreType.DMA((4,)),
            ],
            compiler_params=pltpu.CompilerParams(
                collective_id=0, has_side_effects=True, vmem_limit_bytes=60 * 1024 * 1024
            ),
            cost_estimate=pl.CostEstimate(flops=flops, bytes_accessed=12 << 20, transcendentals=0),
            name="reduce_assemble",
        )(counts, block_map, perms, mass_ii, mass_ib, mass_bb, modes, fixed)

    shared = ("grp", "sub")
    return jax.shard_map(
        per_device,
        mesh=mesh,
        in_specs=(P(shared), P(shared), P(shared, None)) + (P(shared, None, None),) * 5,
        out_specs=(P("grp", "sub", None), P(shared, None, None)),
        check_vma=False,
    )
```

```python
import functools

import jax
import jax.numpy as jnp
from jax import lax
from jax.experimental import pallas as pl
from jax.experimental.pallas import tpu as pltpu
from jax.sharding import PartitionSpec as P

NBG = 16
X_CHIPS = 4
Z_RUN = 4
MESH = pl.DeviceIdType.MESH
PARTS = 4
SIDES = 2
LANES = 128


def contract(left, right):
    return lax.dot_general(left, right, (((0,), (0,)), ((), ())), preferred_element_type=jnp.float32)


def split(value):
    high = value.astype(jnp.bfloat16)
    low = (value - high.astype(jnp.float32)).astype(jnp.bfloat16)
    return high, low


def body(
    n_grp,
    n_sub,
    counts,
    codes_any,
    perms,
    mass_ii,
    mass_ib,
    mass_bb,
    modes,
    fixed,
    blocks,
    coupling,
    m_buf,
    pi_buf,
    b_buf,
    c_buf,
    f_buf,
    perm_buf,
    placed,
    rows_in,
    code_row,
    code_in,
    hot_all,
    staged,
    ahead_in,
    home_in,
    relay_in,
    load_sem,
    part_sem,
    codes_in,
    row_send,
    row_recv,
    code_sem,
    end_sem,
):
    slots, inner, width = mass_ib.shape
    own = width // n_sub
    grp = lax.axis_index("grp")
    sub = lax.axis_index("sub")
    run = n_sub // Z_RUN

    def mirrored(device):
        return (Z_RUN - 1 - device // run) * run + lax.rem(device, run)

    last = lax.rem(grp, X_CHIPS) == X_CHIPS - 1
    first = lax.rem(grp, X_CHIPS) == 0
    next_grp = lax.rem(grp + 1, n_grp)
    prev_grp = lax.rem(grp + n_grp - 1, n_grp)
    out_sub = jnp.where(last, mirrored(sub), sub)
    in_sub = jnp.where(first, mirrored(sub), sub)
    far_grp = lax.rem(grp + X_CHIPS, n_grp)

    def loads(j):
        step = inner // PARTS
        copies = [pltpu.make_async_copy(modes.at[j], c_buf.at[j], load_sem.at[j, 0])]
        for part in range(PARTS):
            rows = pl.ds(part * step, step)
            copies.append(pltpu.make_async_copy(mass_ii.at[j, rows], m_buf.at[j, rows], part_sem.at[j, part]))
        copies.append(pltpu.make_async_copy(mass_ib.at[j], pi_buf.at[j, :, pl.ds(width, width)], load_sem.at[j, 1]))
        copies.append(pltpu.make_async_copy(mass_bb.at[j], b_buf.at[j], load_sem.at[j, 2]))
        copies.append(pltpu.make_async_copy(fixed.at[j], f_buf.at[j], load_sem.at[j, 3]))
        return copies

    for copy in loads(0):
        copy.start()
    small = (
        pltpu.make_async_copy(perms, perm_buf, load_sem.at[0, 4]),
        pltpu.make_async_copy(codes_any, codes_in, load_sem.at[2, 4]),
    )
    for copy in small:
        copy.start()

    barrier = pltpu.get_barrier_semaphore()

    def greet(step, carry):
        peer = lax.rem(sub + step, n_sub)
        pl.semaphore_signal(barrier, inc=1, device_id={"sub": peer}, device_id_type=MESH)
        return carry

    lax.fori_loop(1, n_sub, greet, 0)
    pl.semaphore_signal(barrier, inc=1, device_id={"grp": next_grp, "sub": out_sub}, device_id_type=MESH)
    pl.semaphore_signal(barrier, inc=1, device_id={"grp": prev_grp, "sub": in_sub}, device_id_type=MESH)

    @pl.when(last)
    def _():
        pl.semaphore_signal(barrier, inc=1, device_id={"grp": grp - (X_CHIPS - 1)}, device_id_type=MESH)

    @pl.when(first)
    def _():
        pl.semaphore_signal(barrier, inc=1, device_id={"grp": grp + (X_CHIPS - 1)}, device_id_type=MESH)
        pl.semaphore_signal(barrier, inc=1, device_id={"grp": far_grp}, device_id_type=MESH)

    greeted = n_sub + 1 + jnp.where(last, 1, 0) + jnp.where(first, 2, 0)

    for copy in small:
        copy.wait()
    used = counts[0]
    lane = lax.broadcasted_iota(jnp.int32, (1, 128), 1)
    row = jnp.full((1, 128), -1, jnp.int32)
    for j in range(slots):
        row = jnp.where((lane == j) & (j < used), codes_in[j], row)
    code_row[...] = row
    code_in[0] = row

    def code_copy(step):
        peer = lax.rem(sub + step, n_sub)
        return pltpu.make_async_remote_copy(
            src_ref=code_row,
            dst_ref=code_in.at[step],
            send_sem=code_sem.at[0],
            recv_sem=code_sem.at[1],
            device_id={"sub": peer},
            device_id_type=MESH,
        )

    def left_copy(j, step):
        peer = lax.rem(sub + step, n_sub)
        return pltpu.make_async_remote_copy(
            src_ref=placed.at[0, j, pl.ds(pl.multiple_of(peer * own, own), own)],
            dst_ref=rows_in.at[0, j, pl.ds(pl.multiple_of(step * own, own), own)],
            send_sem=row_send.at[j],
            recv_sem=row_recv.at[j],
            device_id={"sub": peer},
            device_id_type=MESH,
        )

    def right_copy(step):
        peer = lax.rem(sub + step, n_sub)
        block = jnp.where(last, mirrored(peer), peer)
        return pltpu.make_async_remote_copy(
            src_ref=placed.at[1, :, pl.ds(pl.multiple_of(block * own, own), own)],
            dst_ref=rows_in.at[1, :, pl.ds(pl.multiple_of(step * own, own), own)],
            send_sem=row_send.at[slots],
            recv_sem=row_recv.at[slots],
            device_id={"sub": peer},
            device_id_type=MESH,
        )

    row_of = lax.broadcasted_iota(jnp.int32, (width, width), 0)

    def slot(j, carry):
        ready = loads(j)
        step = inner // PARTS
        ready[0].wait()
        for part in range(PARTS):
            ready[1 + part].wait()
            if part == PARTS - 1:

                @pl.when(j + 1 < slots)
                def _():
                    for copy in loads(j + 1):
                        copy.start()

            rows = pl.ds(part * step, step)
            pi_buf[j, rows, pl.ds(0, width)] = jnp.dot(
                m_buf[j, rows], c_buf[j], preferred_element_type=jnp.float32
            ).astype(jnp.bfloat16)
        ready[1 + PARTS].wait()
        ready[2 + PARTS].wait()
        both = contract(c_buf[j], pi_buf[j])
        cross = both[:, width:]
        reduced = both[:, :width] + cross + cross.T + b_buf[j].astype(jnp.float32)
        hot = (row_of == perm_buf[pl.ds(j, 1), :]).astype(jnp.float32).astype(jnp.bfloat16)
        high, low = split(reduced)
        moved_high = jnp.dot(hot, high, preferred_element_type=jnp.float32).astype(jnp.bfloat16)
        moved_low = jnp.dot(hot, low, preferred_element_type=jnp.float32).astype(jnp.bfloat16)
        across = (((1,), (1,)), ((), ()))
        moved = lax.dot_general(
            moved_high, hot, across, preferred_element_type=jnp.float32
        ) + lax.dot_general(moved_low, hot, across, preferred_element_type=jnp.float32)
        for side in range(SIDES):
            placed[side, j] = moved[:, side * LANES : (side + 1) * LANES]

        @pl.when(j == 0)
        def _():
            pl.semaphore_wait(barrier, greeted)
            lax.fori_loop(1, n_sub, lambda step, c: (code_copy(step).start(), c)[1], 0)

        lax.fori_loop(1, n_sub, lambda step, c: (left_copy(j, step).start(), c)[1], 0)
        return carry

    lax.fori_loop(0, slots, slot, 0)

    lax.fori_loop(1, n_sub, lambda step, c: (right_copy(step).start(), c)[1], 0)
    rows_in[0, :, pl.ds(0, own)] = placed[0, :, pl.ds(pl.multiple_of(sub * own, own), own)]
    rows_in[1, :, pl.ds(0, own)] = placed[1, :, pl.ds(pl.multiple_of(out_sub * own, own), own)]

    def couple(j, carry):
        loads(j)[3 + PARTS].wait()
        pair = contract(f_buf[j], pi_buf[j])
        coupling[j] = jnp.where(j < used, pair[:, :width] + pair[:, width:], 0.0)
        return carry

    lax.fori_loop(0, slots, couple, 0)

    others = pltpu.make_async_remote_copy(
        src_ref=code_in.at[pl.ds(1, n_sub - 1)],
        dst_ref=code_in.at[pl.ds(1, n_sub - 1)],
        send_sem=code_sem.at[0],
        recv_sem=code_sem.at[1],
        device_id={"sub": sub},
        device_id_type=MESH,
    )
    others.wait_send()
    others.wait_recv()
    code_all = code_in[...].reshape(n_sub, 128)
    target = lax.broadcasted_iota(jnp.int32, (n_sub, 2 * NBG), 1)
    hot = jnp.concatenate([(code_all[:, j : j + 1] == target).astype(jnp.float32) for j in range(slots)] * 2, axis=0)
    hot_all[...] = hot.T.astype(jnp.bfloat16)

    def arrived(side, j, sem):
        refs = rows_in.at[side, j, pl.ds(own, width - own)]
        copy = pltpu.make_async_remote_copy(
            src_ref=refs,
            dst_ref=refs,
            send_sem=row_send.at[sem],
            recv_sem=row_recv.at[sem],
            device_id={"sub": sub},
            device_id_type=MESH,
        )
        copy.wait_recv()
        copy.wait_send()

    def assemble(side):
        for r in range(0, own, 2):
            terms = []
            for q in (r, r + 1):
                pieces = [split(rows_in[side, j, pl.ds(q, n_sub, stride=own), :]) for j in range(slots)]
                terms.append(jnp.concatenate([p[0] for p in pieces] + [p[1] for p in pieces], axis=0))
            sums = jnp.dot(hot_all[...], jnp.concatenate(terms, axis=1), preferred_element_type=jnp.float32)
            for q in range(2):
                staged[side, pl.ds(r + q, 2 * NBG, stride=own), :] = sums[:, q * LANES : (q + 1) * LANES]

    size = NBG * own

    def end_copy(src, dst, sent, landed, device):
        return pltpu.make_async_remote_copy(
            src_ref=src,
            dst_ref=dst,
            send_sem=end_sem.at[0, sent],
            recv_sem=end_sem.at[1, landed],
            device_id=device,
            device_id_type=MESH,
        )

    def write(side):
        blocks[:, :, pl.ds(side * LANES, LANES)] = (home_in[side] + ahead_in[side]).reshape(NBG, own, LANES)

    def ahead_of(side):
        return staged.at[side, pl.ds(size, size)]

    for j in range(slots):
        arrived(0, j, j)
    assemble(0)
    straight = end_copy(ahead_of(0), ahead_in.at[0], 0, 0, {"grp": next_grp})
    aside = end_copy(ahead_of(0), relay_in, 1, 1, {"grp": grp - (X_CHIPS - 1)})
    onward = end_copy(relay_in, ahead_in.at[0], 4, 0, {"grp": far_grp})

    @pl.when(last)
    def _():
        aside.start()

    @pl.when(jnp.logical_not(last))
    def _():
        straight.start()

    home_in[0] = staged[0, pl.ds(0, size)]

    @pl.when(first)
    def _():
        aside.wait_recv()
        onward.start()

    arrived(1, slice(None), slots)
    assemble(1)
    ahead = end_copy(ahead_of(1), ahead_in.at[1], 2, 2, {"grp": next_grp, "sub": out_sub})
    home = end_copy(staged.at[1, pl.ds(0, size)], home_in.at[1], 3, 3, {"sub": out_sub})
    ahead.start()

    @pl.when(last)
    def _():
        home.start()

    @pl.when(jnp.logical_not(last))
    def _():
        home_in[1] = staged[1, pl.ds(0, size)]

    straight.wait_recv()
    write(0)

    @pl.when(last)
    def _():
        aside.wait_send()
        home.wait()

    @pl.when(jnp.logical_not(last))
    def _():
        straight.wait_send()

    @pl.when(first)
    def _():
        onward.wait_send()

    ahead.wait()
    write(1)


def solution(mesh):
    n_grp, n_sub = mesh.shape["grp"], mesh.shape["sub"]

    def per_device(counts, block_map, perms, mass_ii, mass_ib, mass_bb, modes, fixed):
        slots, inner, width = mass_ib.shape
        k = fixed.shape[2]
        operands = (block_map, perms, mass_ii, mass_ib, mass_bb, modes, fixed)
        own = width // n_sub
        far = pl.BlockSpec(memory_space=pltpu.HBM)
        near = pl.BlockSpec(memory_space=pltpu.VMEM)
        flops = 2 * slots * inner * width * (inner + 2 * width + 2 * k)
        return pl.pallas_call(
            functools.partial(body, n_grp, n_sub),
            out_shape=(
                jax.ShapeDtypeStruct((NBG, own, width), jnp.float32),
                jax.ShapeDtypeStruct((slots, k, width), jnp.float32),
            ),
            in_specs=[pl.BlockSpec(memory_space=pltpu.SMEM)] + [far] * 7,
            out_specs=(near, near),
            scratch_shapes=[
                pltpu.VMEM((slots, inner, inner), jnp.bfloat16),
                pltpu.VMEM((slots, inner, 2 * width), jnp.bfloat16),
                pltpu.VMEM((slots, width, width), jnp.bfloat16),
                pltpu.VMEM((slots, inner, width), jnp.bfloat16),
                pltpu.VMEM((slots, inner, k), jnp.bfloat16),
                pltpu.VMEM((slots, width), jnp.int32),
                pltpu.VMEM((SIDES, slots, width, LANES), jnp.float32),
                pltpu.VMEM((SIDES, slots, width, LANES), jnp.float32),
                pltpu.VMEM((1, 128), jnp.int32),
                pltpu.VMEM((n_sub, 1, 128), jnp.int32),
                pltpu.VMEM((2 * NBG, 2 * slots * n_sub), jnp.bfloat16),
                pltpu.VMEM((SIDES, 2 * NBG * own, LANES), jnp.float32),
                pltpu.VMEM((SIDES, NBG * own, LANES), jnp.float32),
                pltpu.VMEM((SIDES, NBG * own, LANES), jnp.float32),
                pltpu.VMEM((NBG * own, LANES), jnp.float32),
                pltpu.SemaphoreType.DMA((slots, 5)),
                pltpu.SemaphoreType.DMA((slots, PARTS)),
                pltpu.SMEM((slots,), jnp.int32),
                pltpu.SemaphoreType.DMA((slots + 1,)),
                pltpu.SemaphoreType.DMA((slots + 1,)),
                pltpu.SemaphoreType.DMA((2,)),
                pltpu.SemaphoreType.DMA((2, 5)),
            ],
            compiler_params=pltpu.CompilerParams(
                collective_id=0, has_side_effects=True, vmem_limit_bytes=24 * 1024 * 1024
            ),
            cost_estimate=pl.CostEstimate(flops=flops, bytes_accessed=12 << 20, transcendentals=0),
            name="reduce_assemble",
        )(counts, *(pltpu.with_memory_space_constraint(a, pltpu.HBM) for a in operands))

    shared = ("grp", "sub")
    return jax.shard_map(
        per_device,
        mesh=mesh,
        in_specs=(P(shared), P(shared), P(shared, None)) + (P(shared, None, None),) * 5,
        out_specs=(P("grp", "sub", None), P(shared, None, None)),
        check_vma=False,
    )
```

```python
import functools

import jax
import jax.numpy as jnp
from jax import lax
from jax.experimental import pallas as pl
from jax.experimental.pallas import tpu as pltpu
from jax.sharding import PartitionSpec as P

NBG = 16
X_CHIPS = 4
Z_RUN = 4
MESH = pl.DeviceIdType.MESH
PARTS = 2
SIDES = 2
LANES = 128


def contract(left, right):
    return lax.dot_general(left, right, (((0,), (0,)), ((), ())), preferred_element_type=jnp.float32)


def split(value):
    high = value.astype(jnp.bfloat16)
    low = (value - high.astype(jnp.float32)).astype(jnp.bfloat16)
    return high, low


def body(
    n_grp,
    n_sub,
    counts,
    codes_any,
    perms,
    mass_ii,
    mass_ib,
    mass_bb,
    modes,
    fixed,
    blocks,
    coupling,
    m_buf,
    pi_buf,
    b_buf,
    c_buf,
    f_buf,
    perm_buf,
    placed,
    rows_in,
    code_row,
    code_in,
    hot_all,
    staged,
    ahead_in,
    home_in,
    relay_in,
    load_sem,
    part_sem,
    codes_in,
    row_send,
    row_recv,
    code_sem,
    end_sem,
):
    slots, inner, width = mass_ib.shape
    own = width // n_sub
    grp = lax.axis_index("grp")
    sub = lax.axis_index("sub")
    run = n_sub // Z_RUN

    def mirrored(device):
        return (Z_RUN - 1 - device // run) * run + lax.rem(device, run)

    last = lax.rem(grp, X_CHIPS) == X_CHIPS - 1
    first = lax.rem(grp, X_CHIPS) == 0
    next_grp = lax.rem(grp + 1, n_grp)
    prev_grp = lax.rem(grp + n_grp - 1, n_grp)
    out_sub = jnp.where(last, mirrored(sub), sub)
    in_sub = jnp.where(first, mirrored(sub), sub)
    far_grp = lax.rem(grp + X_CHIPS, n_grp)

    def load(j, at):
        pairs = (
            (modes.at[j], c_buf.at[j]),
            (mass_ib.at[j], pi_buf.at[j, :, pl.ds(width, width)]),
            (mass_bb.at[j], b_buf.at[j]),
            (fixed.at[j], f_buf.at[j]),
        )
        return pltpu.make_async_copy(*pairs[at], load_sem.at[j, at])

    def load_part(j, part):
        rows = pl.ds(pl.multiple_of(part * (inner // PARTS), inner // PARTS), inner // PARTS)
        return pltpu.make_async_copy(mass_ii.at[j, rows], m_buf.at[j, rows], part_sem.at[j, part])

    def start_loads(j):
        load(j, 0).start()
        lax.fori_loop(0, PARTS, lambda part, c: (load_part(j, part).start(), c)[1], 0)
        for at in (1, 2, 3):
            load(j, at).start()

    small = (
        pltpu.make_async_copy(codes_any, codes_in, load_sem.at[2, 4]),
        pltpu.make_async_copy(perms, perm_buf, load_sem.at[0, 4]),
    )
    small[1].start()
    start_loads(0)
    small[0].start()

    barrier = pltpu.get_barrier_semaphore()

    def greet(step, carry):
        peer = lax.rem(sub + step, n_sub)
        pl.semaphore_signal(barrier, inc=1, device_id={"sub": peer}, device_id_type=MESH)
        return carry

    lax.fori_loop(1, n_sub, greet, 0)
    pl.semaphore_signal(barrier, inc=1, device_id={"grp": next_grp, "sub": out_sub}, device_id_type=MESH)
    pl.semaphore_signal(barrier, inc=1, device_id={"grp": prev_grp, "sub": in_sub}, device_id_type=MESH)

    @pl.when(last)
    def _():
        pl.semaphore_signal(barrier, inc=1, device_id={"grp": grp - (X_CHIPS - 1)}, device_id_type=MESH)

    @pl.when(first)
    def _():
        pl.semaphore_signal(barrier, inc=1, device_id={"grp": grp + (X_CHIPS - 1)}, device_id_type=MESH)
        pl.semaphore_signal(barrier, inc=1, device_id={"grp": far_grp}, device_id_type=MESH)

    greeted = n_sub + 1 + jnp.where(last, 1, 0) + jnp.where(first, 2, 0)

    used = counts[0]

    def code_copy(step):
        peer = lax.rem(sub + step, n_sub)
        return pltpu.make_async_remote_copy(
            src_ref=code_row,
            dst_ref=code_in.at[step],
            send_sem=code_sem.at[0],
            recv_sem=code_sem.at[1],
            device_id={"sub": peer},
            device_id_type=MESH,
        )

    def left_copy(j, step):
        peer = lax.rem(sub + step, n_sub)
        return pltpu.make_async_remote_copy(
            src_ref=placed.at[0, j, pl.ds(pl.multiple_of(peer * own, own), own)],
            dst_ref=rows_in.at[0, j, pl.ds(pl.multiple_of(step * own, own), own)],
            send_sem=row_send.at[j],
            recv_sem=row_recv.at[j],
            device_id={"sub": peer},
            device_id_type=MESH,
        )

    def right_copy(step):
        peer = lax.rem(sub + step, n_sub)
        block = jnp.where(last, mirrored(peer), peer)
        return pltpu.make_async_remote_copy(
            src_ref=placed.at[1, :, pl.ds(pl.multiple_of(block * own, own), own)],
            dst_ref=rows_in.at[1, :, pl.ds(pl.multiple_of(step * own, own), own)],
            send_sem=row_send.at[slots],
            recv_sem=row_recv.at[slots],
            device_id={"sub": peer},
            device_id_type=MESH,
        )

    small[1].wait()
    row_of = lax.broadcasted_iota(jnp.int32, (width, width), 0)

    def slot(j, carry):
        load(j, 0).wait()

        def product(part, c):
            load_part(j, part).wait()

            @pl.when((part == 0) & (j + 1 < slots))
            def _():
                start_loads(j + 1)

            rows = pl.ds(pl.multiple_of(part * (inner // PARTS), inner // PARTS), inner // PARTS)
            pi_buf[j, rows, pl.ds(0, width)] = jnp.dot(
                m_buf[j, rows], c_buf[j], preferred_element_type=jnp.float32
            ).astype(jnp.bfloat16)
            return c

        lax.fori_loop(0, PARTS, product, 0)
        load(j, 1).wait()
        load(j, 2).wait()
        both = contract(c_buf[j], pi_buf[j])
        cross = both[:, width:]
        reduced = both[:, :width] + cross + cross.T + b_buf[j].astype(jnp.float32)
        hot = (row_of == perm_buf[pl.ds(j, 1), :]).astype(jnp.float32).astype(jnp.bfloat16)
        high, low = split(reduced)
        moved_high = jnp.dot(hot, high, preferred_element_type=jnp.float32).astype(jnp.bfloat16)
        moved_low = jnp.dot(hot, low, preferred_element_type=jnp.float32).astype(jnp.bfloat16)
        across = (((1,), (1,)), ((), ()))
        moved = lax.dot_general(
            moved_high, hot, across, preferred_element_type=jnp.float32
        ) + lax.dot_general(moved_low, hot, across, preferred_element_type=jnp.float32)
        for side in range(SIDES):
            placed[side, j] = moved[:, side * LANES : (side + 1) * LANES]

        @pl.when(j == 0)
        def _():
            small[0].wait()
            lane = lax.broadcasted_iota(jnp.int32, (1, 128), 1)
            row = jnp.full((1, 128), -1, jnp.int32)
            for j in range(slots):
                row = jnp.where((lane == j) & (j < used), codes_in[j], row)
            code_row[...] = row
            code_in[0] = row

            pl.semaphore_wait(barrier, greeted)
            lax.fori_loop(1, n_sub, lambda step, c: (code_copy(step).start(), c)[1], 0)

        lax.fori_loop(1, n_sub, lambda step, c: (left_copy(j, step).start(), c)[1], 0)
        return carry

    lax.fori_loop(0, slots, slot, 0)

    lax.fori_loop(1, n_sub, lambda step, c: (right_copy(step).start(), c)[1], 0)
    rows_in[0, :, pl.ds(0, own)] = placed[0, :, pl.ds(pl.multiple_of(sub * own, own), own)]
    rows_in[1, :, pl.ds(0, own)] = placed[1, :, pl.ds(pl.multiple_of(out_sub * own, own), own)]

    def couple(j, carry):
        load(j, 3).wait()
        pair = contract(f_buf[j], pi_buf[j])
        coupling[j] = jnp.where(j < used, pair[:, :width] + pair[:, width:], 0.0)
        return carry

    lax.fori_loop(0, slots, couple, 0)

    others = pltpu.make_async_remote_copy(
        src_ref=code_in.at[pl.ds(1, n_sub - 1)],
        dst_ref=code_in.at[pl.ds(1, n_sub - 1)],
        send_sem=code_sem.at[0],
        recv_sem=code_sem.at[1],
        device_id={"sub": sub},
        device_id_type=MESH,
    )
    others.wait_send()
    others.wait_recv()
    code_all = code_in[...].reshape(n_sub, 128)
    target = lax.broadcasted_iota(jnp.int32, (n_sub, 2 * NBG), 1)
    hot = jnp.concatenate([(code_all[:, j : j + 1] == target).astype(jnp.float32) for j in range(slots)] * 2, axis=0)
    hot_all[...] = hot.T.astype(jnp.bfloat16)

    def arrived(side, j, sem):
        refs = rows_in.at[side, j, pl.ds(own, width - own)]
        copy = pltpu.make_async_remote_copy(
            src_ref=refs,
            dst_ref=refs,
            send_sem=row_send.at[sem],
            recv_sem=row_recv.at[sem],
            device_id={"sub": sub},
            device_id_type=MESH,
        )
        copy.wait_recv()
        copy.wait_send()

    def assemble(side):
        for r in range(0, own, 2):
            terms = []
            for q in (r, r + 1):
                pieces = [split(rows_in[side, j, pl.ds(q, n_sub, stride=own), :]) for j in range(slots)]
                terms.append(jnp.concatenate([p[0] for p in pieces] + [p[1] for p in pieces], axis=0))
            sums = jnp.dot(hot_all[...], jnp.concatenate(terms, axis=1), preferred_element_type=jnp.float32)
            for q in range(2):
                staged[side, pl.ds(r + q, 2 * NBG, stride=own), :] = sums[:, q * LANES : (q + 1) * LANES]

    size = NBG * own

    def end_copy(src, dst, sent, landed, device):
        return pltpu.make_async_remote_copy(
            src_ref=src,
            dst_ref=dst,
            send_sem=end_sem.at[0, sent],
            recv_sem=end_sem.at[1, landed],
            device_id=device,
            device_id_type=MESH,
        )

    def write(side):
        blocks[:, :, pl.ds(side * LANES, LANES)] = (home_in[side] + ahead_in[side]).reshape(NBG, own, LANES)

    def ahead_of(side):
        return staged.at[side, pl.ds(size, size)]

    for j in range(slots):
        arrived(0, j, j)
    assemble(0)
    straight = end_copy(ahead_of(0), ahead_in.at[0], 0, 0, {"grp": next_grp})
    aside = end_copy(ahead_of(0), relay_in, 1, 1, {"grp": grp - (X_CHIPS - 1)})
    onward = end_copy(relay_in, ahead_in.at[0], 4, 0, {"grp": far_grp})

    @pl.when(last)
    def _():
        aside.start()

    @pl.when(jnp.logical_not(last))
    def _():
        straight.start()

    home_in[0] = staged[0, pl.ds(0, size)]

    @pl.when(first)
    def _():
        aside.wait_recv()
        onward.start()

    arrived(1, slice(None), slots)
    assemble(1)
    ahead = end_copy(ahead_of(1), ahead_in.at[1], 2, 2, {"grp": next_grp, "sub": out_sub})
    home = end_copy(staged.at[1, pl.ds(0, size)], home_in.at[1], 3, 3, {"sub": out_sub})
    ahead.start()

    @pl.when(last)
    def _():
        home.start()

    @pl.when(jnp.logical_not(last))
    def _():
        home_in[1] = staged[1, pl.ds(0, size)]

    straight.wait_recv()
    write(0)

    @pl.when(last)
    def _():
        aside.wait_send()
        home.wait()

    @pl.when(jnp.logical_not(last))
    def _():
        straight.wait_send()

    @pl.when(first)
    def _():
        onward.wait_send()

    ahead.wait()
    write(1)


def finish(blocks_in, coupling_in, blocks, coupling, sems):
    copies = (
        pltpu.make_async_copy(coupling_in, coupling, sems.at[0]),
        pltpu.make_async_copy(blocks_in, blocks, sems.at[1]),
    )
    for copy in copies:
        copy.start()
    for copy in copies:
        copy.wait()


def solution(mesh):
    n_grp, n_sub = mesh.shape["grp"], mesh.shape["sub"]

    def per_device(counts, block_map, perms, mass_ii, mass_ib, mass_bb, modes, fixed):
        slots, inner, width = mass_ib.shape
        k = fixed.shape[2]
        operands = (block_map, perms, mass_ii, mass_ib, mass_bb, modes, fixed)
        own = width // n_sub
        far = pl.BlockSpec(memory_space=pltpu.HBM)
        near = pl.BlockSpec(memory_space=pltpu.VMEM)
        flops = 2 * slots * inner * width * (inner + 2 * width + 2 * k)
        shapes = (
            jax.ShapeDtypeStruct((NBG, own, width), jnp.float32),
            jax.ShapeDtypeStruct((slots, k, width), jnp.float32),
        )
        made = pl.pallas_call(
            functools.partial(body, n_grp, n_sub),
            out_shape=shapes,
            in_specs=[pl.BlockSpec(memory_space=pltpu.SMEM)] + [far] * 7,
            out_specs=(near, near),
            scratch_shapes=[
                pltpu.VMEM((slots, inner, inner), jnp.bfloat16),
                pltpu.VMEM((slots, inner, 2 * width), jnp.bfloat16),
                pltpu.VMEM((slots, width, width), jnp.bfloat16),
                pltpu.VMEM((slots, inner, width), jnp.bfloat16),
                pltpu.VMEM((slots, inner, k), jnp.bfloat16),
                pltpu.VMEM((slots, width), jnp.int32),
                pltpu.VMEM((SIDES, slots, width, LANES), jnp.float32),
                pltpu.VMEM((SIDES, slots, width, LANES), jnp.float32),
                pltpu.VMEM((1, 128), jnp.int32),
                pltpu.VMEM((n_sub, 1, 128), jnp.int32),
                pltpu.VMEM((2 * NBG, 2 * slots * n_sub), jnp.bfloat16),
                pltpu.VMEM((SIDES, 2 * NBG * own, LANES), jnp.float32),
                pltpu.VMEM((SIDES, NBG * own, LANES), jnp.float32),
                pltpu.VMEM((SIDES, NBG * own, LANES), jnp.float32),
                pltpu.VMEM((NBG * own, LANES), jnp.float32),
                pltpu.SemaphoreType.DMA((slots, 5)),
                pltpu.SemaphoreType.DMA((slots, PARTS)),
                pltpu.SMEM((slots,), jnp.int32),
                pltpu.SemaphoreType.DMA((slots + 1,)),
                pltpu.SemaphoreType.DMA((slots + 1,)),
                pltpu.SemaphoreType.DMA((2,)),
                pltpu.SemaphoreType.DMA((2, 5)),
            ],
            compiler_params=pltpu.CompilerParams(
                collective_id=0, has_side_effects=True, vmem_limit_bytes=24 * 1024 * 1024
            ),
            cost_estimate=pl.CostEstimate(flops=flops, bytes_accessed=12 << 20, transcendentals=0),
            name="reduce_assemble",
        )(counts, *(pltpu.with_memory_space_constraint(a, pltpu.HBM) for a in operands))
        return pl.pallas_call(
            finish,
            out_shape=shapes,
            in_specs=[near] * 2,
            out_specs=(pl.BlockSpec(memory_space=pl.ANY),) * 2,
            scratch_shapes=[pltpu.SemaphoreType.DMA((2,))],
            compiler_params=pltpu.CompilerParams(vmem_limit_bytes=4 * 1024 * 1024),
            name="finish",
        )(*made)

    shared = ("grp", "sub")
    return jax.shard_map(
        per_device,
        mesh=mesh,
        in_specs=(P(shared), P(shared), P(shared, None)) + (P(shared, None, None),) * 5,
        out_specs=(P("grp", "sub", None), P(shared, None, None)),
        check_vma=False,
    )
```

```python
import functools

import jax
import jax.numpy as jnp
from jax import lax
from jax.experimental import pallas as pl
from jax.experimental.pallas import tpu as pltpu
from jax.sharding import PartitionSpec as P

NBG = 16
X_CHIPS = 4
Z_RUN = 4
MESH = pl.DeviceIdType.MESH
PARTS = 2
SIDES = 2
LANES = 128


def contract(left, right):
    return lax.dot_general(left, right, (((0,), (0,)), ((), ())), preferred_element_type=jnp.float32)


def split(value):
    high = value.astype(jnp.bfloat16)
    low = (value - high.astype(jnp.float32)).astype(jnp.bfloat16)
    return high, low


def body(
    n_grp,
    n_sub,
    counts,
    codes_any,
    perms,
    mass_ii,
    mass_ib,
    mass_bb,
    modes,
    fixed,
    blocks,
    coupling,
    m_buf,
    pi_buf,
    b_buf,
    c_buf,
    f_buf,
    perm_buf,
    placed,
    rows_in,
    code_row,
    code_in,
    hot_all,
    staged,
    ahead_in,
    home_in,
    relay_in,
    carried,
    load_sem,
    part_sem,
    codes_in,
    row_send,
    row_recv,
    code_sem,
    end_sem,
    carry_sem,
):
    slots, inner, width = mass_ib.shape
    own = width // n_sub
    grp = lax.axis_index("grp")
    sub = lax.axis_index("sub")
    run = n_sub // Z_RUN

    def mirrored(device):
        return (Z_RUN - 1 - device // run) * run + lax.rem(device, run)

    last = lax.rem(grp, X_CHIPS) == X_CHIPS - 1
    first = lax.rem(grp, X_CHIPS) == 0
    next_grp = lax.rem(grp + 1, n_grp)
    prev_grp = lax.rem(grp + n_grp - 1, n_grp)
    out_sub = jnp.where(last, mirrored(sub), sub)
    in_sub = jnp.where(first, mirrored(sub), sub)
    far_grp = lax.rem(grp + X_CHIPS, n_grp)
    carrier = lax.rem(grp, X_CHIPS) == X_CHIPS - 2
    side_size = n_sub // 2
    far_low = side_size - (sub // side_size) * side_size

    def near_peer(turn):
        return side_size - far_low + lax.rem(sub + turn, side_size)

    def far_peer(turn):
        return far_low + lax.rem(sub + turn, side_size)

    def load(j, at):
        pairs = (
            (modes.at[j], c_buf.at[j]),
            (mass_ib.at[j], pi_buf.at[j, :, pl.ds(width, width)]),
            (mass_bb.at[j], b_buf.at[j]),
            (fixed.at[j], f_buf.at[j]),
        )
        return pltpu.make_async_copy(*pairs[at], load_sem.at[j, at])

    def load_part(j, part):
        rows = pl.ds(pl.multiple_of(part * (inner // PARTS), inner // PARTS), inner // PARTS)
        return pltpu.make_async_copy(mass_ii.at[j, rows], m_buf.at[j, rows], part_sem.at[j, part])

    def start_loads(j):
        load(j, 0).start()
        lax.fori_loop(0, PARTS, lambda part, c: (load_part(j, part).start(), c)[1], 0)
        for at in (1, 2, 3):
            load(j, at).start()

    small = (
        pltpu.make_async_copy(codes_any, codes_in, load_sem.at[2, 4]),
        pltpu.make_async_copy(perms, perm_buf, load_sem.at[0, 4]),
    )
    small[1].start()
    start_loads(0)
    small[0].start()

    barrier = pltpu.get_barrier_semaphore()

    def greet(step, carry):
        peer = lax.rem(sub + step, n_sub)
        pl.semaphore_signal(barrier, inc=1, device_id={"sub": peer}, device_id_type=MESH)
        return carry

    lax.fori_loop(1, n_sub, greet, 0)
    pl.semaphore_signal(barrier, inc=1, device_id={"grp": next_grp, "sub": out_sub}, device_id_type=MESH)
    pl.semaphore_signal(barrier, inc=1, device_id={"grp": prev_grp, "sub": in_sub}, device_id_type=MESH)

    @pl.when(last)
    def _():
        pl.semaphore_signal(barrier, inc=1, device_id={"grp": grp - (X_CHIPS - 1)}, device_id_type=MESH)

    @pl.when(first)
    def _():
        pl.semaphore_signal(barrier, inc=1, device_id={"grp": grp + (X_CHIPS - 1)}, device_id_type=MESH)
        pl.semaphore_signal(barrier, inc=1, device_id={"grp": far_grp}, device_id_type=MESH)

    def greet_far(shift):
        def one(turn, carry):
            device = {"grp": grp + shift, "sub": far_peer(turn)}
            pl.semaphore_signal(barrier, inc=1, device_id=device, device_id_type=MESH)
            return carry

        lax.fori_loop(0, side_size, one, 0)

    @pl.when(carrier)
    def _():
        greet_far(1)

    @pl.when(last)
    def _():
        greet_far(-1)

    greeted = n_sub + 1 + jnp.where(last, 1, 0) + jnp.where(first, 2, 0)
    greeted += jnp.where(carrier | last, side_size, 0)

    used = counts[0]

    def code_copy(step):
        peer = lax.rem(sub + step, n_sub)
        return pltpu.make_async_remote_copy(
            src_ref=code_row,
            dst_ref=code_in.at[step],
            send_sem=code_sem.at[0],
            recv_sem=code_sem.at[1],
            device_id={"sub": peer},
            device_id_type=MESH,
        )

    def left_copy(j, step):
        peer = lax.rem(sub + step, n_sub)
        return pltpu.make_async_remote_copy(
            src_ref=placed.at[0, j, pl.ds(pl.multiple_of(peer * own, own), own)],
            dst_ref=rows_in.at[0, j, pl.ds(pl.multiple_of(step * own, own), own)],
            send_sem=row_send.at[j],
            recv_sem=row_recv.at[j],
            device_id={"sub": peer},
            device_id_type=MESH,
        )

    def right_copy(peer, count, sem):
        step = lax.rem(peer - sub + n_sub, n_sub)
        block = jnp.where(last, mirrored(peer), peer)
        return pltpu.make_async_remote_copy(
            src_ref=placed.at[1, pl.ds(0, count), pl.ds(pl.multiple_of(block * own, own), own)],
            dst_ref=rows_in.at[1, pl.ds(0, count), pl.ds(pl.multiple_of(step * own, own), own)],
            send_sem=row_send.at[sem],
            recv_sem=row_recv.at[slots],
            device_id={"sub": peer},
            device_id_type=MESH,
        )

    carry_low = (side_size - far_low) * own
    carry_size = side_size * own

    carry_out = pltpu.make_async_remote_copy(
        src_ref=placed.at[1, slots - 1, pl.ds(pl.multiple_of(carry_low, own), carry_size)],
        dst_ref=carried,
        send_sem=carry_sem.at[0],
        recv_sem=carry_sem.at[1],
        device_id={"grp": grp - 1},
        device_id_type=MESH,
    )

    def carry_on(turn):
        peer = far_peer(turn)
        step = lax.rem(peer - sub + n_sub, n_sub)
        return pltpu.make_async_remote_copy(
            src_ref=carried.at[pl.ds(pl.multiple_of(mirrored(peer) * own - carry_low, own), own)],
            dst_ref=rows_in.at[1, slots - 1, pl.ds(pl.multiple_of(step * own, own), own)],
            send_sem=carry_sem.at[2],
            recv_sem=row_recv.at[slots],
            device_id={"grp": grp + 1, "sub": peer},
            device_id_type=MESH,
        )

    small[1].wait()
    row_of = lax.broadcasted_iota(jnp.int32, (width, width), 0)

    def slot(j, carry):
        load(j, 0).wait()

        def product(part, c):
            load_part(j, part).wait()

            @pl.when((part == 0) & (j + 1 < slots))
            def _():
                start_loads(j + 1)

            rows = pl.ds(pl.multiple_of(part * (inner // PARTS), inner // PARTS), inner // PARTS)
            pi_buf[j, rows, pl.ds(0, width)] = jnp.dot(
                m_buf[j, rows], c_buf[j], preferred_element_type=jnp.float32
            ).astype(jnp.bfloat16)
            return c

        lax.fori_loop(0, PARTS, product, 0)
        load(j, 1).wait()
        load(j, 2).wait()
        both = contract(c_buf[j], pi_buf[j])
        cross = both[:, width:]
        reduced = both[:, :width] + cross + cross.T + b_buf[j].astype(jnp.float32)
        hot = (row_of == perm_buf[pl.ds(j, 1), :]).astype(jnp.float32).astype(jnp.bfloat16)
        high, low = split(reduced)
        moved_high = jnp.dot(hot, high, preferred_element_type=jnp.float32).astype(jnp.bfloat16)
        moved_low = jnp.dot(hot, low, preferred_element_type=jnp.float32).astype(jnp.bfloat16)
        across = (((1,), (1,)), ((), ()))
        moved = lax.dot_general(
            moved_high, hot, across, preferred_element_type=jnp.float32
        ) + lax.dot_general(moved_low, hot, across, preferred_element_type=jnp.float32)
        for side in range(SIDES):
            placed[side, j] = moved[:, side * LANES : (side + 1) * LANES]

        @pl.when(j == 0)
        def _():
            small[0].wait()
            lane = lax.broadcasted_iota(jnp.int32, (1, 128), 1)
            row = jnp.full((1, 128), -1, jnp.int32)
            for j in range(slots):
                row = jnp.where((lane == j) & (j < used), codes_in[j], row)
            code_row[...] = row
            code_in[0] = row

            pl.semaphore_wait(barrier, greeted)
            lax.fori_loop(1, n_sub, lambda step, c: (code_copy(step).start(), c)[1], 0)

        lax.fori_loop(1, n_sub, lambda step, c: (left_copy(j, step).start(), c)[1], 0)
        return carry

    lax.fori_loop(0, slots, slot, 0)

    @pl.when(last)
    def _():
        carry_out.start()

    rows_in[0, :, pl.ds(0, own)] = placed[0, :, pl.ds(pl.multiple_of(sub * own, own), own)]
    rows_in[1, :, pl.ds(0, own)] = placed[1, :, pl.ds(pl.multiple_of(out_sub * own, own), own)]

    def couple(j, carry):
        load(j, 3).wait()
        pair = contract(f_buf[j], pi_buf[j])
        coupling[j] = jnp.where(j < used, pair[:, :width] + pair[:, width:], 0.0)
        return carry

    lax.fori_loop(0, slots, couple, 0)

    @pl.when(carrier)
    def _():
        carry_out.wait_recv()
        lax.fori_loop(0, side_size, lambda turn, c: (carry_on(turn).start(), c)[1], 0)

    lax.fori_loop(1, side_size, lambda turn, c: (right_copy(near_peer(turn), slots, slots).start(), c)[1], 0)

    @pl.when(carrier)
    def _():
        pltpu.make_async_remote_copy(
            src_ref=carried,
            dst_ref=carried,
            send_sem=carry_sem.at[2],
            recv_sem=carry_sem.at[1],
            device_id={"sub": sub},
            device_id_type=MESH,
        ).wait_send()

    def far_rows(count):
        return lambda turn, c: (right_copy(far_peer(turn), count, slots + 1).start(), c)[1]

    @pl.when(last)
    def _():
        lax.fori_loop(0, side_size, far_rows(slots - 1), 0)

    @pl.when(jnp.logical_not(last))
    def _():
        lax.fori_loop(0, side_size, far_rows(slots), 0)


    others = pltpu.make_async_remote_copy(
        src_ref=code_in.at[pl.ds(1, n_sub - 1)],
        dst_ref=code_in.at[pl.ds(1, n_sub - 1)],
        send_sem=code_sem.at[0],
        recv_sem=code_sem.at[1],
        device_id={"sub": sub},
        device_id_type=MESH,
    )
    others.wait_send()
    others.wait_recv()
    code_all = code_in[...].reshape(n_sub, 128)
    target = lax.broadcasted_iota(jnp.int32, (n_sub, 2 * NBG), 1)
    hot = jnp.concatenate([(code_all[:, j : j + 1] == target).astype(jnp.float32) for j in range(slots)] * 2, axis=0)
    hot_all[...] = hot.T.astype(jnp.bfloat16)

    def expect(refs, sem):
        return pltpu.make_async_remote_copy(
            src_ref=refs,
            dst_ref=refs,
            send_sem=row_send.at[sem],
            recv_sem=row_recv.at[sem],
            device_id={"sub": sub},
            device_id_type=MESH,
        )

    def assemble(side):
        for r in range(0, own, 2):
            terms = []
            for q in (r, r + 1):
                pieces = [split(rows_in[side, j, pl.ds(q, n_sub, stride=own), :]) for j in range(slots)]
                terms.append(jnp.concatenate([p[0] for p in pieces] + [p[1] for p in pieces], axis=0))
            sums = jnp.dot(hot_all[...], jnp.concatenate(terms, axis=1), preferred_element_type=jnp.float32)
            for q in range(2):
                staged[side, pl.ds(r + q, 2 * NBG, stride=own), :] = sums[:, q * LANES : (q + 1) * LANES]

    size = NBG * own

    def end_copy(src, dst, sent, landed, device):
        return pltpu.make_async_remote_copy(
            src_ref=src,
            dst_ref=dst,
            send_sem=end_sem.at[0, sent],
            recv_sem=end_sem.at[1, landed],
            device_id=device,
            device_id_type=MESH,
        )

    def write(side):
        blocks[:, :, pl.ds(side * LANES, LANES)] = (home_in[side] + ahead_in[side]).reshape(NBG, own, LANES)

    def ahead_of(side):
        return staged.at[side, pl.ds(size, size)]

    for j in range(slots):
        left = expect(rows_in.at[0, j, pl.ds(own, width - own)], j)
        left.wait_recv()
        left.wait_send()
    assemble(0)
    straight = end_copy(ahead_of(0), ahead_in.at[0], 0, 0, {"grp": next_grp})
    aside = end_copy(ahead_of(0), relay_in, 1, 1, {"grp": grp - (X_CHIPS - 1)})
    onward = end_copy(relay_in, ahead_in.at[0], 4, 0, {"grp": far_grp})

    @pl.when(last)
    def _():
        aside.start()

    @pl.when(jnp.logical_not(last))
    def _():
        straight.start()

    home_in[0] = staged[0, pl.ds(0, size)]

    @pl.when(first)
    def _():
        aside.wait_recv()
        onward.start()

    expect(rows_in.at[1, :, pl.ds(own, width - own)], slots).wait_recv()
    assemble(1)
    ahead = end_copy(ahead_of(1), ahead_in.at[1], 2, 2, {"grp": next_grp, "sub": out_sub})
    home = end_copy(staged.at[1, pl.ds(0, size)], home_in.at[1], 3, 3, {"sub": out_sub})
    ahead.start()

    @pl.when(last)
    def _():
        home.start()

    @pl.when(jnp.logical_not(last))
    def _():
        home_in[1] = staged[1, pl.ds(0, size)]

    straight.wait_recv()
    write(0)

    @pl.when(last)
    def _():
        aside.wait_send()
        home.wait()

    @pl.when(jnp.logical_not(last))
    def _():
        straight.wait_send()

    @pl.when(first)
    def _():
        onward.wait_send()

    ahead.wait()
    write(1)
    expect(rows_in.at[1, :, pl.ds(own, (side_size - 1) * own)], slots).wait_send()

    @pl.when(last)
    def _():
        expect(rows_in.at[1, pl.ds(0, slots - 1), pl.ds(0, carry_size)], slots + 1).wait_send()
        carry_out.wait_send()

    @pl.when(jnp.logical_not(last))
    def _():
        expect(rows_in.at[1, :, pl.ds(0, carry_size)], slots + 1).wait_send()


def finish(blocks_in, coupling_in, blocks, coupling, sems):
    copies = (
        pltpu.make_async_copy(coupling_in, coupling, sems.at[0]),
        pltpu.make_async_copy(blocks_in, blocks, sems.at[1]),
    )
    for copy in copies:
        copy.start()
    for copy in copies:
        copy.wait()


def solution(mesh):
    n_grp, n_sub = mesh.shape["grp"], mesh.shape["sub"]

    def per_device(counts, block_map, perms, mass_ii, mass_ib, mass_bb, modes, fixed):
        slots, inner, width = mass_ib.shape
        k = fixed.shape[2]
        operands = (block_map, perms, mass_ii, mass_ib, mass_bb, modes, fixed)
        own = width // n_sub
        far = pl.BlockSpec(memory_space=pltpu.HBM)
        near = pl.BlockSpec(memory_space=pltpu.VMEM)
        flops = 2 * slots * inner * width * (inner + 2 * width + 2 * k)
        shapes = (
            jax.ShapeDtypeStruct((NBG, own, width), jnp.float32),
            jax.ShapeDtypeStruct((slots, k, width), jnp.float32),
        )
        made = pl.pallas_call(
            functools.partial(body, n_grp, n_sub),
            out_shape=shapes,
            in_specs=[pl.BlockSpec(memory_space=pltpu.SMEM)] + [far] * 7,
            out_specs=(near, near),
            scratch_shapes=[
                pltpu.VMEM((slots, inner, inner), jnp.bfloat16),
                pltpu.VMEM((slots, inner, 2 * width), jnp.bfloat16),
                pltpu.VMEM((slots, width, width), jnp.bfloat16),
                pltpu.VMEM((slots, inner, width), jnp.bfloat16),
                pltpu.VMEM((slots, inner, k), jnp.bfloat16),
                pltpu.VMEM((slots, width), jnp.int32),
                pltpu.VMEM((SIDES, slots, width, LANES), jnp.float32),
                pltpu.VMEM((SIDES, slots, width, LANES), jnp.float32),
                pltpu.VMEM((1, 128), jnp.int32),
                pltpu.VMEM((n_sub, 1, 128), jnp.int32),
                pltpu.VMEM((2 * NBG, 2 * slots * n_sub), jnp.bfloat16),
                pltpu.VMEM((SIDES, 2 * NBG * own, LANES), jnp.float32),
                pltpu.VMEM((SIDES, NBG * own, LANES), jnp.float32),
                pltpu.VMEM((SIDES, NBG * own, LANES), jnp.float32),
                pltpu.VMEM((NBG * own, LANES), jnp.float32),
                pltpu.VMEM((width // 2, LANES), jnp.float32),
                pltpu.SemaphoreType.DMA((slots, 5)),
                pltpu.SemaphoreType.DMA((slots, PARTS)),
                pltpu.SMEM((slots,), jnp.int32),
                pltpu.SemaphoreType.DMA((slots + 2,)),
                pltpu.SemaphoreType.DMA((slots + 1,)),
                pltpu.SemaphoreType.DMA((2,)),
                pltpu.SemaphoreType.DMA((2, 5)),
                pltpu.SemaphoreType.DMA((3,)),
            ],
            compiler_params=pltpu.CompilerParams(
                collective_id=0, has_side_effects=True, vmem_limit_bytes=24 * 1024 * 1024
            ),
            cost_estimate=pl.CostEstimate(flops=flops, bytes_accessed=12 << 20, transcendentals=0),
            name="reduce_assemble",
        )(counts, *(pltpu.with_memory_space_constraint(a, pltpu.HBM) for a in operands))
        return pl.pallas_call(
            finish,
            out_shape=shapes,
            in_specs=[near] * 2,
            out_specs=(pl.BlockSpec(memory_space=pl.ANY),) * 2,
            scratch_shapes=[pltpu.SemaphoreType.DMA((2,))],
            compiler_params=pltpu.CompilerParams(vmem_limit_bytes=4 * 1024 * 1024),
            name="finish",
        )(*made)

    shared = ("grp", "sub")
    return jax.shard_map(
        per_device,
        mesh=mesh,
        in_specs=(P(shared), P(shared), P(shared, None)) + (P(shared, None, None),) * 5,
        out_specs=(P("grp", "sub", None), P(shared, None, None)),
        check_vma=False,
    )
```

```python
import functools

import jax
import jax.numpy as jnp
from jax import lax
from jax.experimental import pallas as pl
from jax.experimental.pallas import tpu as pltpu
from jax.sharding import PartitionSpec as P

NBG = 16
X_CHIPS = 4
Z_RUN = 4
MESH = pl.DeviceIdType.MESH
PARTS = 2
SIDES = 2
LANES = 128


def contract(left, right):
    return lax.dot_general(left, right, (((0,), (0,)), ((), ())), preferred_element_type=jnp.float32)


def split(value):
    high = value.astype(jnp.bfloat16)
    low = (value - high.astype(jnp.float32)).astype(jnp.bfloat16)
    return high, low


def body(
    n_grp,
    n_sub,
    counts,
    codes_any,
    perms,
    mass_ii,
    mass_ib,
    mass_bb,
    modes,
    fixed,
    blocks,
    coupling,
    m_buf,
    pi_buf,
    b_buf,
    c_buf,
    f_buf,
    perm_buf,
    placed,
    rows_in,
    code_row,
    code_in,
    hot_all,
    staged,
    ahead_in,
    home_in,
    relay_in,
    carried,
    load_sem,
    part_sem,
    codes_in,
    row_send,
    row_recv,
    code_sem,
    end_sem,
    carry_sem,
):
    slots, inner, width = mass_ib.shape
    own = width // n_sub
    grp = lax.axis_index("grp")
    sub = lax.axis_index("sub")
    run = n_sub // Z_RUN

    def mirrored(device):
        return (Z_RUN - 1 - device // run) * run + lax.rem(device, run)

    last = lax.rem(grp, X_CHIPS) == X_CHIPS - 1
    first = lax.rem(grp, X_CHIPS) == 0
    next_grp = lax.rem(grp + 1, n_grp)
    prev_grp = lax.rem(grp + n_grp - 1, n_grp)
    out_sub = jnp.where(last, mirrored(sub), sub)
    in_sub = jnp.where(first, mirrored(sub), sub)
    far_grp = lax.rem(grp + X_CHIPS, n_grp)
    beside = (sub // run + 1 - 2 * lax.rem(sub // run, 2)) * run + lax.rem(sub, run)
    carrier = lax.rem(grp, X_CHIPS) == X_CHIPS - 2
    side_size = n_sub // 2
    far_low = side_size - (sub // side_size) * side_size

    def near_peer(turn):
        return side_size - far_low + lax.rem(sub + turn, side_size)

    def far_peer(turn):
        return far_low + lax.rem(sub + turn, side_size)

    def load(j, at):
        pairs = (
            (modes.at[j], c_buf.at[j]),
            (mass_ib.at[j], pi_buf.at[j, :, pl.ds(width, width)]),
            (mass_bb.at[j], b_buf.at[j]),
            (fixed.at[j], f_buf.at[j]),
        )
        return pltpu.make_async_copy(*pairs[at], load_sem.at[j, at])

    def load_part(j, part):
        rows = pl.ds(pl.multiple_of(part * (inner // PARTS), inner // PARTS), inner // PARTS)
        return pltpu.make_async_copy(mass_ii.at[j, rows], m_buf.at[j, rows], part_sem.at[j, part])

    def start_loads(j):
        load(j, 0).start()
        lax.fori_loop(0, PARTS, lambda part, c: (load_part(j, part).start(), c)[1], 0)
        for at in (1, 2, 3):
            load(j, at).start()

    small = (
        pltpu.make_async_copy(codes_any, codes_in, load_sem.at[2, 4]),
        pltpu.make_async_copy(perms, perm_buf, load_sem.at[0, 4]),
    )
    small[1].start()
    start_loads(0)
    small[0].start()

    barrier = pltpu.get_barrier_semaphore()

    def greet(step, carry):
        peer = lax.rem(sub + step, n_sub)
        pl.semaphore_signal(barrier, inc=1, device_id={"sub": peer}, device_id_type=MESH)
        return carry

    lax.fori_loop(1, n_sub, greet, 0)
    pl.semaphore_signal(barrier, inc=1, device_id={"grp": next_grp, "sub": out_sub}, device_id_type=MESH)
    pl.semaphore_signal(barrier, inc=1, device_id={"grp": prev_grp, "sub": in_sub}, device_id_type=MESH)

    @pl.when(last)
    def _():
        pl.semaphore_signal(barrier, inc=1, device_id={"grp": grp - (X_CHIPS - 1), "sub": beside}, device_id_type=MESH)

    @pl.when(first)
    def _():
        pl.semaphore_signal(barrier, inc=1, device_id={"grp": grp + (X_CHIPS - 1), "sub": beside}, device_id_type=MESH)
        pl.semaphore_signal(barrier, inc=1, device_id={"grp": far_grp, "sub": beside}, device_id_type=MESH)

    def greet_far(shift):
        def one(turn, carry):
            device = {"grp": grp + shift, "sub": far_peer(turn)}
            pl.semaphore_signal(barrier, inc=1, device_id=device, device_id_type=MESH)
            return carry

        lax.fori_loop(0, side_size, one, 0)

    @pl.when(carrier)
    def _():
        greet_far(1)

    @pl.when(last)
    def _():
        greet_far(-1)

    greeted = n_sub + 1 + jnp.where(last, 1, 0) + jnp.where(first, 2, 0)
    greeted += jnp.where(carrier | last, side_size, 0)

    used = counts[0]

    def code_copy(step):
        peer = lax.rem(sub + step, n_sub)
        return pltpu.make_async_remote_copy(
            src_ref=code_row,
            dst_ref=code_in.at[step],
            send_sem=code_sem.at[0],
            recv_sem=code_sem.at[1],
            device_id={"sub": peer},
            device_id_type=MESH,
        )

    def left_copy(j, step):
        peer = lax.rem(sub + step, n_sub)
        return pltpu.make_async_remote_copy(
            src_ref=placed.at[0, j, pl.ds(pl.multiple_of(peer * own, own), own)],
            dst_ref=rows_in.at[0, j, pl.ds(pl.multiple_of(step * own, own), own)],
            send_sem=row_send.at[j],
            recv_sem=row_recv.at[j],
            device_id={"sub": peer},
            device_id_type=MESH,
        )

    def right_copy(peer, count, sem):
        step = lax.rem(peer - sub + n_sub, n_sub)
        block = jnp.where(last, mirrored(peer), peer)
        return pltpu.make_async_remote_copy(
            src_ref=placed.at[1, pl.ds(0, count), pl.ds(pl.multiple_of(block * own, own), own)],
            dst_ref=rows_in.at[1, pl.ds(0, count), pl.ds(pl.multiple_of(step * own, own), own)],
            send_sem=row_send.at[sem],
            recv_sem=row_recv.at[slots],
            device_id={"sub": peer},
            device_id_type=MESH,
        )

    carry_low = (side_size - far_low) * own
    carry_size = side_size * own

    carry_out = pltpu.make_async_remote_copy(
        src_ref=placed.at[1, slots - 1, pl.ds(pl.multiple_of(carry_low, own), carry_size)],
        dst_ref=carried,
        send_sem=carry_sem.at[0],
        recv_sem=carry_sem.at[1],
        device_id={"grp": grp - 1},
        device_id_type=MESH,
    )

    def carry_on(turn):
        peer = far_peer(turn)
        step = lax.rem(peer - sub + n_sub, n_sub)
        return pltpu.make_async_remote_copy(
            src_ref=carried.at[pl.ds(pl.multiple_of(mirrored(peer) * own - carry_low, own), own)],
            dst_ref=rows_in.at[1, slots - 1, pl.ds(pl.multiple_of(step * own, own), own)],
            send_sem=carry_sem.at[2],
            recv_sem=row_recv.at[slots],
            device_id={"grp": grp + 1, "sub": peer},
            device_id_type=MESH,
        )

    small[1].wait()
    row_of = lax.broadcasted_iota(jnp.int32, (width, width), 0)

    def slot(j, carry):
        load(j, 0).wait()

        def product(part, c):
            load_part(j, part).wait()

            @pl.when((part == 0) & (j + 1 < slots))
            def _():
                start_loads(j + 1)

            rows = pl.ds(pl.multiple_of(part * (inner // PARTS), inner // PARTS), inner // PARTS)
            pi_buf[j, rows, pl.ds(0, width)] = jnp.dot(
                m_buf[j, rows], c_buf[j], preferred_element_type=jnp.float32
            ).astype(jnp.bfloat16)
            return c

        lax.fori_loop(0, PARTS, product, 0)
        load(j, 1).wait()
        load(j, 2).wait()
        both = contract(c_buf[j], pi_buf[j])
        cross = both[:, width:]
        reduced = both[:, :width] + cross + cross.T + b_buf[j].astype(jnp.float32)
        hot = (row_of == perm_buf[pl.ds(j, 1), :]).astype(jnp.float32).astype(jnp.bfloat16)
        high, low = split(reduced)
        moved_high = jnp.dot(hot, high, preferred_element_type=jnp.float32).astype(jnp.bfloat16)
        moved_low = jnp.dot(hot, low, preferred_element_type=jnp.float32).astype(jnp.bfloat16)
        across = (((1,), (1,)), ((), ()))
        moved = lax.dot_general(
            moved_high, hot, across, preferred_element_type=jnp.float32
        ) + lax.dot_general(moved_low, hot, across, preferred_element_type=jnp.float32)
        for side in range(SIDES):
            placed[side, j] = moved[:, side * LANES : (side + 1) * LANES]

        @pl.when(j == 0)
        def _():
            small[0].wait()
            lane = lax.broadcasted_iota(jnp.int32, (1, 128), 1)
            row = jnp.full((1, 128), -1, jnp.int32)
            for j in range(slots):
                row = jnp.where((lane == j) & (j < used), codes_in[j], row)
            code_row[...] = row
            code_in[0] = row

            pl.semaphore_wait(barrier, greeted)
            lax.fori_loop(1, n_sub, lambda step, c: (code_copy(step).start(), c)[1], 0)

        lax.fori_loop(1, n_sub, lambda step, c: (left_copy(j, step).start(), c)[1], 0)
        return carry

    lax.fori_loop(0, slots, slot, 0)

    @pl.when(last)
    def _():
        carry_out.start()

    rows_in[0, :, pl.ds(0, own)] = placed[0, :, pl.ds(pl.multiple_of(sub * own, own), own)]
    rows_in[1, :, pl.ds(0, own)] = placed[1, :, pl.ds(pl.multiple_of(out_sub * own, own), own)]

    def couple(j, carry):
        load(j, 3).wait()
        pair = contract(f_buf[j], pi_buf[j])
        coupling[j] = jnp.where(j < used, pair[:, :width] + pair[:, width:], 0.0)
        return carry

    lax.fori_loop(0, slots, couple, 0)

    @pl.when(carrier)
    def _():
        carry_out.wait_recv()
        lax.fori_loop(0, side_size, lambda turn, c: (carry_on(turn).start(), c)[1], 0)

    lax.fori_loop(1, side_size, lambda turn, c: (right_copy(near_peer(turn), slots, slots).start(), c)[1], 0)

    @pl.when(carrier)
    def _():
        pltpu.make_async_remote_copy(
            src_ref=carried,
            dst_ref=carried,
            send_sem=carry_sem.at[2],
            recv_sem=carry_sem.at[1],
            device_id={"sub": sub},
            device_id_type=MESH,
        ).wait_send()

    def far_rows(count):
        return lambda turn, c: (right_copy(far_peer(turn), count, slots + 1).start(), c)[1]

    @pl.when(last)
    def _():
        lax.fori_loop(0, side_size, far_rows(slots - 1), 0)

    @pl.when(jnp.logical_not(last))
    def _():
        lax.fori_loop(0, side_size, far_rows(slots), 0)


    others = pltpu.make_async_remote_copy(
        src_ref=code_in.at[pl.ds(1, n_sub - 1)],
        dst_ref=code_in.at[pl.ds(1, n_sub - 1)],
        send_sem=code_sem.at[0],
        recv_sem=code_sem.at[1],
        device_id={"sub": sub},
        device_id_type=MESH,
    )
    others.wait_send()
    others.wait_recv()
    code_all = code_in[...].reshape(n_sub, 128)
    target = lax.broadcasted_iota(jnp.int32, (n_sub, 2 * NBG), 1)
    hot = jnp.concatenate([(code_all[:, j : j + 1] == target).astype(jnp.float32) for j in range(slots)] * 2, axis=0)
    hot_all[...] = hot.T.astype(jnp.bfloat16)

    def expect(refs, sem):
        return pltpu.make_async_remote_copy(
            src_ref=refs,
            dst_ref=refs,
            send_sem=row_send.at[sem],
            recv_sem=row_recv.at[sem],
            device_id={"sub": sub},
            device_id_type=MESH,
        )

    def assemble(side):
        for r in range(0, own, 2):
            terms = []
            for q in (r, r + 1):
                pieces = [split(rows_in[side, j, pl.ds(q, n_sub, stride=own), :]) for j in range(slots)]
                terms.append(jnp.concatenate([p[0] for p in pieces] + [p[1] for p in pieces], axis=0))
            sums = jnp.dot(hot_all[...], jnp.concatenate(terms, axis=1), preferred_element_type=jnp.float32)
            for q in range(2):
                staged[side, pl.ds(r + q, 2 * NBG, stride=own), :] = sums[:, q * LANES : (q + 1) * LANES]

    size = NBG * own

    def end_copy(src, dst, sent, landed, device):
        return pltpu.make_async_remote_copy(
            src_ref=src,
            dst_ref=dst,
            send_sem=end_sem.at[0, sent],
            recv_sem=end_sem.at[1, landed],
            device_id=device,
            device_id_type=MESH,
        )

    def write(side):
        blocks[:, :, pl.ds(side * LANES, LANES)] = (home_in[side] + ahead_in[side]).reshape(NBG, own, LANES)

    def ahead_of(side):
        return staged.at[side, pl.ds(size, size)]

    for j in range(slots):
        left = expect(rows_in.at[0, j, pl.ds(own, width - own)], j)
        left.wait_recv()
        left.wait_send()
    assemble(0)
    straight = end_copy(ahead_of(0), ahead_in.at[0], 0, 0, {"grp": next_grp})
    aside = end_copy(ahead_of(0), relay_in, 1, 1, {"grp": grp - (X_CHIPS - 1), "sub": beside})
    onward = end_copy(relay_in, ahead_in.at[0], 4, 0, {"grp": far_grp, "sub": beside})

    @pl.when(last)
    def _():
        aside.start()

    @pl.when(jnp.logical_not(last))
    def _():
        straight.start()

    home_in[0] = staged[0, pl.ds(0, size)]

    @pl.when(first)
    def _():
        aside.wait_recv()
        onward.start()

    expect(rows_in.at[1, :, pl.ds(own, width - own)], slots).wait_recv()
    assemble(1)
    ahead = end_copy(ahead_of(1), ahead_in.at[1], 2, 2, {"grp": next_grp, "sub": out_sub})
    home = end_copy(staged.at[1, pl.ds(0, size)], home_in.at[1], 3, 3, {"sub": out_sub})
    ahead.start()

    @pl.when(last)
    def _():
        home.start()

    @pl.when(jnp.logical_not(last))
    def _():
        home_in[1] = staged[1, pl.ds(0, size)]

    straight.wait_recv()
    write(0)

    @pl.when(last)
    def _():
        aside.wait_send()
        home.wait()

    @pl.when(jnp.logical_not(last))
    def _():
        straight.wait_send()

    @pl.when(first)
    def _():
        onward.wait_send()

    ahead.wait()
    write(1)
    expect(rows_in.at[1, :, pl.ds(own, (side_size - 1) * own)], slots).wait_send()

    @pl.when(last)
    def _():
        expect(rows_in.at[1, pl.ds(0, slots - 1), pl.ds(0, carry_size)], slots + 1).wait_send()
        carry_out.wait_send()

    @pl.when(jnp.logical_not(last))
    def _():
        expect(rows_in.at[1, :, pl.ds(0, carry_size)], slots + 1).wait_send()


def finish(blocks_in, coupling_in, blocks, coupling, sems):
    copies = (
        pltpu.make_async_copy(coupling_in, coupling, sems.at[0]),
        pltpu.make_async_copy(blocks_in, blocks, sems.at[1]),
    )
    for copy in copies:
        copy.start()
    for copy in copies:
        copy.wait()


def solution(mesh):
    n_grp, n_sub = mesh.shape["grp"], mesh.shape["sub"]

    def per_device(counts, block_map, perms, mass_ii, mass_ib, mass_bb, modes, fixed):
        slots, inner, width = mass_ib.shape
        k = fixed.shape[2]
        operands = (block_map, perms, mass_ii, mass_ib, mass_bb, modes, fixed)
        own = width // n_sub
        far = pl.BlockSpec(memory_space=pltpu.HBM)
        near = pl.BlockSpec(memory_space=pltpu.VMEM)
        flops = 2 * slots * inner * width * (inner + 2 * width + 2 * k)
        shapes = (
            jax.ShapeDtypeStruct((NBG, own, width), jnp.float32),
            jax.ShapeDtypeStruct((slots, k, width), jnp.float32),
        )
        made = pl.pallas_call(
            functools.partial(body, n_grp, n_sub),
            out_shape=shapes,
            in_specs=[pl.BlockSpec(memory_space=pltpu.SMEM)] + [far] * 7,
            out_specs=(near, near),
            scratch_shapes=[
                pltpu.VMEM((slots, inner, inner), jnp.bfloat16),
                pltpu.VMEM((slots, inner, 2 * width), jnp.bfloat16),
                pltpu.VMEM((slots, width, width), jnp.bfloat16),
                pltpu.VMEM((slots, inner, width), jnp.bfloat16),
                pltpu.VMEM((slots, inner, k), jnp.bfloat16),
                pltpu.VMEM((slots, width), jnp.int32),
                pltpu.VMEM((SIDES, slots, width, LANES), jnp.float32),
                pltpu.VMEM((SIDES, slots, width, LANES), jnp.float32),
                pltpu.VMEM((1, 128), jnp.int32),
                pltpu.VMEM((n_sub, 1, 128), jnp.int32),
                pltpu.VMEM((2 * NBG, 2 * slots * n_sub), jnp.bfloat16),
                pltpu.VMEM((SIDES, 2 * NBG * own, LANES), jnp.float32),
                pltpu.VMEM((SIDES, NBG * own, LANES), jnp.float32),
                pltpu.VMEM((SIDES, NBG * own, LANES), jnp.float32),
                pltpu.VMEM((NBG * own, LANES), jnp.float32),
                pltpu.VMEM((width // 2, LANES), jnp.float32),
                pltpu.SemaphoreType.DMA((slots, 5)),
                pltpu.SemaphoreType.DMA((slots, PARTS)),
                pltpu.SMEM((slots,), jnp.int32),
                pltpu.SemaphoreType.DMA((slots + 2,)),
                pltpu.SemaphoreType.DMA((slots + 1,)),
                pltpu.SemaphoreType.DMA((2,)),
                pltpu.SemaphoreType.DMA((2, 5)),
                pltpu.SemaphoreType.DMA((3,)),
            ],
            compiler_params=pltpu.CompilerParams(
                collective_id=0, has_side_effects=True, vmem_limit_bytes=24 * 1024 * 1024
            ),
            cost_estimate=pl.CostEstimate(flops=flops, bytes_accessed=12 << 20, transcendentals=0),
            name="reduce_assemble",
        )(counts, *(pltpu.with_memory_space_constraint(a, pltpu.HBM) for a in operands))
        return pl.pallas_call(
            finish,
            out_shape=shapes,
            in_specs=[near] * 2,
            out_specs=(pl.BlockSpec(memory_space=pl.ANY),) * 2,
            scratch_shapes=[pltpu.SemaphoreType.DMA((2,))],
            compiler_params=pltpu.CompilerParams(vmem_limit_bytes=4 * 1024 * 1024),
            name="finish",
        )(*made)

    shared = ("grp", "sub")
    return jax.shard_map(
        per_device,
        mesh=mesh,
        in_specs=(P(shared), P(shared), P(shared, None)) + (P(shared, None, None),) * 5,
        out_specs=(P("grp", "sub", None), P(shared, None, None)),
        check_vma=False,
    )
```
